256 devices in a mesh: rows: 64 (over x, z, core), cols: 4 (over y).
Axes of the slice: x: 4, y: 4, z: 8, core: 2. Of those that a mesh axis runs over, the one named last changes fastest.
Arguments:
- matrix: bfloat16 [131072, 1024], P('rows', 'cols'), as said below
- row_signs: int32 [131072], P('rows'), may hold values from 0 to 1
- sampled_rows: int32 [64, 2048], P('rows'), may hold values from 0 to 2047
- right_sides: float32 [8, 131072], P(None, 'rows'), may hold values from -6 to 6
Outputs:
- solution: float32 [8, 1024], P(None, 'cols')
- residual: float32 [8, 131072], P(None, 'rows')
The draws below stay inside these ranges and needn't reach their ends.
Inputs may be any that keep to these rules, and one draw needn't show every extreme that they name: `matrix`: entries are at most 70 / sqrt(131072) in magnitude.
All inputs are finite; a program needn't handle non-finite values.
Results may differ from the reference program's by a relative error of at most 0.0013.
Values sent between devices are 32-bit elements; how exact they have to be, the bound alone decides.
No kernel may reach another device: no remote copies, remote signals or barrier semaphores. Data moves between devices by JAX's collectives and lax.ppermute only.
A program may use at most 64 MiB of HBM per device.

```python
import math
import jax
import jax.numpy as jnp
from jax import lax

UNKNOWNS = 1024
SKETCH = 2048
SYSTEMS = 8
ROUNDS = 2
BLOCK_ROWS = 2048
BLOCKS = 64
EQUATIONS = 131072


def column_mixer(mix_key):
    square = jax.random.normal(mix_key, (UNKNOWNS, UNKNOWNS), jnp.float32)
    basis, _ = jnp.linalg.qr(square)
    ladder = jnp.exp(jnp.linspace(0.0, math.log(30.0), UNKNOWNS).astype(jnp.float32))
    ladder = ladder / jnp.sqrt(jnp.mean(ladder * ladder))
    return jnp.dot(basis * ladder[None, :], basis.T)


def draw_matrix(key, part):
    noise_key = jax.random.fold_in(jax.random.fold_in(key, 17), 0)
    scale_key = jax.random.fold_in(jax.random.fold_in(key, 17), 1)
    mix_key = jax.random.fold_in(jax.random.fold_in(key, 17), 3)
    scales = jnp.exp(jax.random.uniform(scale_key, (BLOCKS, 1, UNKNOWNS), jnp.float32) * math.log(10.0))
    base = jnp.clip(jax.random.normal(noise_key, (BLOCKS, BLOCK_ROWS, UNKNOWNS), jnp.float32), -4.0, 4.0)
    scaled = (base * scales).reshape(EQUATIONS, UNKNOWNS)
    mixed = jnp.dot(scaled, column_mixer(mix_key))
    result = jnp.clip(mixed, -60.0, 60.0) / math.sqrt(EQUATIONS)
    return result.astype(jnp.bfloat16)


def with_ends(array, rng, smallest, top_value):
    place = [jax.random.randint(jax.random.fold_in(rng, axis), (), 0, length) for axis, length in enumerate(array.shape)]
    longest = array.shape.index(max(array.shape))
    next_to = place[:longest] + [(place[longest] + 1) % array.shape[longest]] + place[longest + 1:]
    return array.at[tuple(place)].set(smallest).at[tuple(next_to)].set(top_value)


def shard_levels(stream_key, dims, shards, low, top_value):
    def one(position, blocks):
        draws = jax.random.uniform(jax.random.fold_in(jax.random.fold_in(stream_key, 6), position), (blocks,), jnp.float32, low / len(shards), top_value / len(shards))
        return jnp.repeat(jnp.exp(draws), dims[position] // blocks).reshape((-1,) + (1,) * (len(dims) - position - 1))

    level = one(*shards[0])
    for cut in shards[1:]:
        level = level * one(*cut)
    return level


def scatter_about(key, dims, spread, bound, cuts=(), kind=jnp.bfloat16):
    factor_of = shard_levels(key, dims, cuts, -0.22, 0.18) if cuts else 1.0
    values = jax.random.normal(key, dims, jnp.float32) * spread * factor_of
    return jnp.minimum(jnp.maximum(values, -bound), bound).astype(kind)


def setup_inputs(seed: int = 0) -> dict:
    splits = jax.random.split(jax.random.key(seed), 5)
    return {
        "matrix": draw_matrix(jax.random.fold_in(splits[4], 71), 0),
        "row_signs": with_ends(jax.random.randint(splits[1], (EQUATIONS,), 0, 2), jax.random.fold_in(splits[1], 1), 0, 1).astype(jnp.int32),
        "sampled_rows": with_ends(jax.random.randint(splits[2], (BLOCKS, SKETCH), 0, BLOCK_ROWS), jax.random.fold_in(splits[2], 1), 0, BLOCK_ROWS - 1).astype(jnp.int32),
        "right_sides": scatter_about(splits[3], (SYSTEMS, EQUATIONS), 1.0, 6.0, ((1, 64),), jnp.float32),
    }


highest = lax.Precision.HIGHEST

def sylvester(matrix_order):
    positions = jnp.arange(matrix_order, dtype=jnp.int32)
    common = jnp.bitwise_and(positions[:, None], positions[None, :])
    parity = jnp.zeros((matrix_order, matrix_order), jnp.int32)
    for bit_place in range(max(matrix_order.bit_length() - 1, 0)):
        parity = parity + jnp.bitwise_and(jnp.right_shift(common, bit_place), 1)
    return jnp.where(jnp.bitwise_and(parity, 1) == 0, 1.0, -1.0).astype(jnp.float32)

def hadamard(signed):
    row_count, col_count = signed.shape
    bit_count = row_count.bit_length() - 1
    factor_sizes = []
    while bit_count > 0:
        group_bits = min(4, bit_count)
        factor_sizes.append(2 ** group_bits)
        bit_count = bit_count - group_bits
    result = signed
    for factor_size in factor_sizes:
        shaped = result.reshape(factor_size, row_count // factor_size, col_count)
        result = jnp.einsum('ab,bmn->man', sylvester(factor_size), shaped, precision=highest).reshape(row_count, col_count)
    return result

def solve_right(factor, vectors):
    return lax.linalg.triangular_solve(factor, vectors, left_side=False, lower=True, transpose_a=True)

def solve_left(factor, vectors):
    return lax.linalg.triangular_solve(factor, vectors, left_side=False, lower=True, transpose_a=False)

def reference(matrix, row_signs, sampled_rows, right_sides):
    row_blocks = matrix.reshape(BLOCKS, BLOCK_ROWS, UNKNOWNS)
    sign_blocks = (1 - 2 * row_signs).reshape(BLOCKS, BLOCK_ROWS)
    systems = right_sides.shape[0]

    def sketch_step(running, scan_item):
        row_block, sign_column, sample_row = scan_item
        signed = row_block.astype(jnp.float32) * sign_column.astype(jnp.float32)[:, None]
        mixed_rows = hadamard(signed)
        picked = jnp.take(mixed_rows, sample_row, axis=0) * (1.0 / math.sqrt(SKETCH))
        return (running + picked, None)
    sketch, _ = lax.scan(sketch_step, jnp.zeros((SKETCH, UNKNOWNS), jnp.float32), (row_blocks, sign_blocks, sampled_rows))
    gram_matrix = jnp.dot(sketch.T, sketch, precision=highest)
    factor = jnp.linalg.cholesky(gram_matrix)

    def forward(vectors):

        def one_block(row_block):
            return lax.dot_general(vectors, row_block.astype(jnp.float32), (((1,), (1,)), ((), ())), precision=highest)
        pieces = lax.map(one_block, row_blocks)
        return jnp.transpose(pieces, (1, 0, 2)).reshape(systems, EQUATIONS)

    def backward(vectors):
        split = jnp.transpose(vectors.reshape(systems, BLOCKS, BLOCK_ROWS), (1, 0, 2))

        def add_block(running, scan_item):
            row_block, part_rows = scan_item
            return (running + jnp.dot(part_rows, row_block.astype(jnp.float32), precision=highest), None)
        summed, _ = lax.scan(add_block, jnp.zeros((systems, UNKNOWNS), jnp.float32), (row_blocks, split))
        return summed
    beta_norm = jnp.sqrt(lax.optimization_barrier(jnp.sum(right_sides * right_sides, axis=1)))
    left_unit = right_sides / beta_norm[:, None]
    back_rest = solve_right(factor, backward(left_unit))
    alpha_norm = jnp.sqrt(lax.optimization_barrier(jnp.sum(back_rest * back_rest, axis=1)))
    right_unit = back_rest / alpha_norm[:, None]
    search = right_unit
    coeffs = jnp.zeros((systems, UNKNOWNS), jnp.float32)
    phibar = beta_norm
    rhobar = alpha_norm
    for iteration in range(ROUNDS):
        forward_rest = forward(solve_left(factor, right_unit)) - alpha_norm[:, None] * left_unit
        beta_norm = jnp.sqrt(lax.optimization_barrier(jnp.sum(forward_rest * forward_rest, axis=1)))
        left_unit = forward_rest / beta_norm[:, None]
        back_rest = solve_right(factor, backward(left_unit)) - beta_norm[:, None] * right_unit
        alpha_norm = jnp.sqrt(lax.optimization_barrier(jnp.sum(back_rest * back_rest, axis=1)))
        right_unit = back_rest / alpha_norm[:, None]
        rho_total = jnp.sqrt(rhobar * rhobar + beta_norm * beta_norm)
        cosine = rhobar / rho_total
        sine_part = beta_norm / rho_total
        theta_term = sine_part * alpha_norm
        rhobar = -cosine * alpha_norm
        phi_term = cosine * phibar
        phibar = sine_part * phibar
        coeffs = coeffs + (phi_term / rho_total)[:, None] * search
        search = right_unit - (theta_term / rho_total)[:, None] * search
    solution = solve_left(factor, coeffs)
    residual = right_sides - forward(solution)
    return (solution, residual)
```

```python
import math

import jax
import jax.numpy as jnp
from jax import lax
from jax.experimental import pallas as pl
from jax.experimental.pallas import tpu as pltpu
from jax.sharding import PartitionSpec as P

SKETCH = 2048
ROUNDS = 2
f32 = jnp.float32
highest = lax.Precision.HIGHEST
HI = lax.Precision.HIGHEST
N, B, SUB = 1024, 128, 8
NB = N // B

def mm(a, b, ca, cb):
    return lax.dot_general(a, b, (((ca,), (cb,)), ((), ())), precision=HI, preferred_element_type=jnp.float32)

def eliminate_block(tiles):
    count = len(tiles)
    lane = lax.broadcasted_iota(jnp.int32, (SUB, B), 1)
    sub = lax.broadcasted_iota(jnp.int32, (SUB, B), 0)
    spread = lambda x, j: jnp.broadcast_to(x[:, j:j + 1], (SUB, B))
    row = lambda x, r: jnp.broadcast_to(x[r:r + 1, :], (SUB, B))
    unit, scaled = [], []
    tiles = list(tiles)
    for p in range(count):
        at = SUB * p
        x = tiles[p]
        cols = [spread(x, at + r) for r in range(SUB)]
        inside = (lane >= at) & (lane < at + SUB)
        eye = jnp.where(lane - at == sub, 1.0, 0.0).astype(jnp.float32)
        unit.append(jnp.where(lane < at, x, eye))
        y = jnp.where(inside, eye, x)
        for r in range(SUB):
            inv = 1.0 / row(cols[r], r)
            here = sub == r
            def step(v):
                t = row(v, r) * inv
                return jnp.where(here, t, v - cols[r] * t)
            for j in range(r + 1, SUB):
                cols[j] = step(cols[j])
            y = step(y)
        scaled.append(jnp.where(lane < at + SUB, y, 0.0))
        rows = [row(y, q) for q in range(SUB)]
        for t in range(p + 1, count):
            z = jnp.where(inside, 0.0, tiles[t])
            for q in range(SUB):
                z = z - spread(tiles[t], at + q) * rows[q]
            tiles[t] = z
    return unit, scaled

def back_substitute(w_of, strips_ref, both_ref, out_ref):
    for k in reversed(range(NB)):
        acc = w_of(k)
        if k + 1 < NB:
            acc = acc - mm(out_ref[:, (k + 1) * B:], strips_ref[k * B:(k + 1) * B, (k + 1) * B:], 1, 1)
        out_ref[:, k * B:(k + 1) * B] = mm(acc, both_ref[k, :B, :], 1, 0)

def solve_kernel(strips_ref, both_ref, rhs_ref, out_ref, g, w):
    g[...] = rhs_ref[...]
    for k in range(NB):
        lo, hi = k * B, (k + 1) * B
        vw = mm(g[:, lo:hi], both_ref[k], 1, 1)
        w[:, lo:hi] = vw[:, B:]
        if k + 1 < NB:
            g[:, hi:] = g[:, hi:] - mm(vw[:, :B], strips_ref[lo:hi, hi:], 1, 0)
    back_substitute(lambda k: w[:, k * B:(k + 1) * B], strips_ref, both_ref, out_ref)


PIECE = 160
STACK = 8 * PIECE
VM = pl.BlockSpec(memory_space=pltpu.VMEM)
SM = pl.BlockSpec(memory_space=pltpu.SMEM)


def shape(*dims):
    return jax.ShapeDtypeStruct(dims, f32)


def params():
    return pltpu.CompilerParams(vmem_limit_bytes=48 << 20)


def blocks_of(c):
    nxt, far = (c + 1) % 4, (c + 2) % 4
    lo, hi = min(c, nxt), max(c, nxt)
    low, high = min(c, far), max(c, far)
    own = [(2 * c, 2 * c), (2 * c, 2 * c + 1), (2 * c + 1, 2 * c + 1)]
    near = [(2 * lo + i, 2 * hi + j) for i in (0, 1) for j in (0, 1)]
    side = [(2 * low + (0 if c < 2 else 1), 2 * high + j) for j in (0, 1)]
    return own + near + side


def gram_kernel(where_ref, own_ref, next_ref, far_ref, back_ref, square_ref, out_ref):
    c = where_ref[3]
    own, nxt, far = own_ref[...], next_ref[...], far_ref[...]
    mine = mm(own, own, 0, 0)
    out_ref[0:B] = mine[:B, :B]
    out_ref[B:2 * B] = mine[:B, B:]
    out_ref[2 * B:3 * B] = mine[B:, B:]
    wraps = c == 3
    near = mm(jnp.where(wraps, nxt, own), jnp.where(wraps, own, nxt), 0, 0)
    for i in range(2):
        for j in range(2):
            at = (3 + 2 * i + j) * B
            out_ref[at:at + B] = near[i * B:(i + 1) * B, j * B:(j + 1) * B]
    first = c < 2
    low = jnp.where(first, own[:, :B], far[:, B:])
    side = mm(low, jnp.where(first, far, own), 0, 0)
    for j in range(2):
        out_ref[(7 + j) * B:(8 + j) * B] = side[:, j * B:(j + 1) * B]
    out_ref[9 * B:] = jnp.zeros((B, B), f32)
    out_ref[9 * B:9 * B + 8] = back_ref[:, :B]
    out_ref[9 * B + 8:9 * B + 16] = back_ref[:, B:]
    out_ref[9 * B + 16:9 * B + 24] = jnp.broadcast_to(square_ref[...], (8, B))


def assemble(where_ref, pieces_ref, work, rhs_ref, norm_ref):
    core, first, second, c = where_ref[0], where_ref[1], where_ref[2], where_ref[3]
    first_other, second_other = where_ref[4], where_ref[5]

    def copy(ca, row, rows, store):
        place = (ca - c) & 3
        done = 0
        while done < rows:
            piece, inner = divmod(row + done, PIECE)
            count = min(rows - done, PIECE - inner)
            other = (piece >> 2) ^ core
            one = ((piece >> 1) & 1) ^ jnp.where(other == 0, first, first_other)
            two = (piece & 1) ^ jnp.where(other == 0, second, second_other)
            if piece >> 2:
                two = two ^ one
            at = other * 4 + one * 2 + two
            store(done, count, pieces_ref[at, place, inner:inner + count, :])
            done += count

    for ca in range(4):
        for n, (i, j) in enumerate(blocks_of(ca)):
            def store(done, count, value, i=i, j=j):
                work[i * B + done:i * B + done + count, j * B:(j + 1) * B] = value
            copy(ca, n * B, B, store)
        for h in range(2):
            def keep(done, count, value, ca=ca, h=h):
                rhs_ref[:, (2 * ca + h) * B:(2 * ca + h + 1) * B] = value
            copy(ca, 9 * B + 8 * h, 8, keep)

    def put(done, count, value):
        norm_ref[...] = value
    copy(0, 9 * B + 16, 8, put)


def factor_kernel(where_ref, pieces_ref, strips_ref, both_ref, rhs_ref, norm_ref, out_ref, work, diag, g, w):
    assemble(where_ref, pieces_ref, work, rhs_ref, norm_ref)
    g[...] = rhs_ref[...]
    diag[...] = work[:B, :B]

    def body(k, carry):
        unit, scaled = eliminate_block([diag[SUB * t:SUB * (t + 1), :] for t in range(B // SUB)])
        for t in range(B // SUB):
            both_ref[k, SUB * t:SUB * (t + 1), :] = unit[t]
            both_ref[k, B + SUB * t:B + SUB * (t + 1), :] = scaled[t]
        for kk in range(NB):
            @pl.when(k == kk)
            def _():
                lo, hi = kk * B, (kk + 1) * B
                both = both_ref[kk]
                vw = mm(g[:, lo:hi], both, 1, 1)
                w[:, lo:hi] = vw[:, B:]
                if kk + 1 < NB:
                    pair = mm(both, work[lo:hi, hi:], 1, 0)
                    strip = pair[B:]
                    strips_ref[lo:hi, hi:] = strip
                    left = pair[:B]
                    g[:, hi:] = g[:, hi:] - mm(vw[:, :B], strip, 1, 0)
                    for i in range(kk + 1, NB):
                        off = (i - kk - 1) * B
                        new = work[i * B:(i + 1) * B, i * B:] - mm(left[:, off:off + B], strip[:, off:], 0, 0)
                        work[i * B:(i + 1) * B, i * B:] = new
                        if i == kk + 1:
                            diag[...] = new[:, :B]
        return carry

    lax.fori_loop(0, NB, body, 0)
    back_substitute(lambda k: w[:, k * B:(k + 1) * B], strips_ref, both_ref, out_ref)


def gram_pieces(where, own, nxt, far, back, squares):
    return pl.pallas_call(
        gram_kernel, in_specs=[SM] + [VM] * 5, out_specs=VM, out_shape=shape(STACK, B), compiler_params=params()
    )(where, own, nxt, far, back, squares)


def factor_and_solve(where, pieces):
    rows = pltpu.VMEM((8, N), f32)
    return pl.pallas_call(
        factor_kernel,
        in_specs=[SM, VM],
        out_specs=[VM] * 5,
        out_shape=[shape(N, N), shape(NB, 2 * B, B), shape(8, N), shape(8, B), shape(8, N)],
        scratch_shapes=[pltpu.VMEM((N, N), f32), pltpu.VMEM((B, B), f32), rows, rows],
        compiler_params=params(),
    )(where, pieces)


def solve_again(strips, both, rhs):
    rows = pltpu.VMEM((8, N), f32)
    return pl.pallas_call(
        solve_kernel, in_specs=[VM] * 3, out_specs=VM, out_shape=shape(8, N),
        scratch_shapes=[rows, rows], compiler_params=params(),
    )(strips, both, rhs)


def sylvester(matrix_order):
    positions = jnp.arange(matrix_order, dtype=jnp.int32)
    common = jnp.bitwise_and(positions[:, None], positions[None, :])
    parity = jnp.zeros((matrix_order, matrix_order), jnp.int32)
    for bit_place in range(max(matrix_order.bit_length() - 1, 0)):
        parity = parity + jnp.bitwise_and(jnp.right_shift(common, bit_place), 1)
    return jnp.where(jnp.bitwise_and(parity, 1) == 0, 1.0, -1.0).astype(jnp.float32)


def transform(signed):
    row_count, col_count = signed.shape
    bit_count = row_count.bit_length() - 1
    outer_order = 2 ** (bit_count - bit_count // 2)
    inner_order = row_count // outer_order
    section_one = jnp.dot(
        sylvester(outer_order).astype(jnp.bfloat16),
        signed.reshape(outer_order, inner_order * col_count),
        preferred_element_type=jnp.float32,
    )
    second = jnp.einsum(
        "cd,adn->acn",
        sylvester(inner_order),
        section_one.reshape(outer_order, inner_order, col_count),
        precision=highest,
    )
    return second.reshape(row_count, col_count)


def row_perm(x_flip, z_flip):
    pairs = []
    for i in range(64):
        core, z, x = i & 1, (i >> 1) & 7, i >> 4
        zz = (z - core) & 7
        zz ^= z_flip
        z2 = (zz + core) & 7
        x2 = x ^ x_flip[core]
        pairs.append((i, x2 * 16 + z2 * 2 + core))
    return pairs


CORE = [(i, i ^ 1) for i in range(64)]
XA = row_perm((1, 3), 0)
XB = row_perm((3, 1), 0)
Z1, Z2, Z4 = (row_perm((0, 0), m) for m in (1, 2, 4))


def halve(v, perm, bit):
    half = v.shape[0] // 2
    send = lax.dynamic_slice_in_dim(v, (1 - bit) * half, half, 0)
    keep = lax.dynamic_slice_in_dim(v, bit * half, half, 0)
    return keep + lax.ppermute(send, "rows", perm)


def with_partner(v, perm, axis="rows"):
    return v + lax.ppermute(v, axis, perm)


def over_rows(v):
    for perm in (CORE, XA, XB, Z1, Z2, Z4):
        v = with_partner(v, perm)
    return v


def over_cols(v):
    v = with_partner(v, [(i, i ^ 1) for i in range(4)], "cols")
    return with_partner(v, [(i, i ^ 3) for i in range(4)], "cols")


def from_right(v, k):
    return lax.ppermute(v, "cols", [(i, (i - k) % 4) for i in range(4)])


def local(matrix, row_signs, sampled_rows, right_sides):
    row_count, col_count = matrix.shape
    place = lax.axis_index("rows")
    c = lax.axis_index("cols")
    core, z, x = place & 1, (place >> 1) & 7, place >> 4
    zz = (z - core) & 7
    gray, high, low = (x ^ (x >> 1)) & 1, x >> 1, x & 1
    first = jnp.where(core == 0, gray, high)
    second = jnp.where(core == 0, high, low)
    first_other = jnp.where(core == 0, high, gray)
    second_other = jnp.where(core == 0, low, high)
    where = jnp.stack([core, first, second, c, first_other, second_other]).astype(jnp.int32)

    wide = matrix.astype(f32)
    flipped = (1 - 2 * row_signs).astype(jnp.bfloat16)
    signed = matrix * flipped[:, None]
    mixed_rows = transform(signed)
    piece = jnp.take(mixed_rows, sampled_rows[0], axis=0) * (1.0 / math.sqrt(SKETCH))
    for perm, bit in (
        (CORE, core), (XA, first), (XB, second), (Z1, zz & 1), (Z2, (zz >> 1) & 1), (Z4, zz >> 2),
    ):
        piece = halve(piece, perm, bit)

    def backward(vectors):
        return jnp.dot(vectors, wide, precision=highest)

    def squares(vectors):
        return jnp.sum(vectors * vectors, axis=1, keepdims=True)

    def forward(vectors):
        own_part = lax.dynamic_slice_in_dim(vectors, c * col_count, col_count, 1)
        part = lax.dot_general(own_part, wide, (((1,), (1,)), ((), ())), precision=highest)
        return over_cols(part)

    stack = gram_pieces(
        where, piece, from_right(piece, 1), from_right(piece, 2), backward(right_sides), squares(right_sides)
    )
    for perm, bit in ((CORE, core), (XA, first), (XB, second)):
        stack = halve(stack, perm, bit)
    for perm in (Z1, Z2, Z4):
        stack = with_partner(stack, perm)
    parts = jnp.stack([stack] + [from_right(stack, k) for k in (1, 2, 3)])
    for perm in (XB, XA, CORE):
        parts = jnp.stack([parts, lax.ppermute(parts, "rows", perm)])
    pieces = parts.reshape(8, 4, PIECE, B)
    strips, both, gradient, norms, solved = factor_and_solve(where, pieces)

    beta = jnp.sqrt(norms[:, :1])
    left = right_sides / beta
    rest, point = gradient / beta, solved / beta
    alpha = jnp.sqrt(jnp.sum(rest * point, axis=1, keepdims=True))
    h, point = rest / alpha, point / alpha
    search, search_image = point, None
    total = jnp.zeros_like(point)
    image = jnp.zeros_like(right_sides)
    phibar, rhobar, turn = beta, alpha, None
    for round_number in range(ROUNDS):
        point_image = forward(point)
        search_image = point_image if turn is None else point_image - turn * search_image
        rest_left = point_image - alpha * left
        if round_number + 1 < ROUNDS:
            packed = jnp.concatenate(
                [backward(rest_left), jnp.broadcast_to(squares(rest_left), (rest_left.shape[0], B))], axis=1
            )
            packed = over_rows(packed)
            beta = jnp.sqrt(packed[:, col_count:col_count + 1])
            own = packed[:, :col_count] / beta
            around = jnp.concatenate([own] + [from_right(own, k) for k in (1, 2, 3)], axis=1)
            whole = lax.dynamic_slice_in_dim(
                jnp.concatenate([around, around], axis=1), (4 - c) * col_count, 4 * col_count, 1
            )
            left = rest_left / beta
            rest = whole - beta * h
            point = solve_again(strips, both, rest)
            alpha_next = jnp.sqrt(jnp.sum(rest * point, axis=1, keepdims=True))
            h, point = rest / alpha_next, point / alpha_next
        else:
            every = lax.all_to_all(
                jnp.broadcast_to(squares(rest_left).reshape(1, 1, -1), (64, 1, rest_left.shape[0])), "rows", 0, 0, tiled=True
            )
            beta = jnp.sqrt(jnp.sum(every, axis=0).reshape(-1, 1))
            alpha_next = alpha
        rho = jnp.sqrt(rhobar * rhobar + beta * beta)
        cosine = rhobar / rho
        sine = beta / rho
        theta = sine * alpha_next
        rhobar = -cosine * alpha_next
        phi = cosine * phibar
        phibar = sine * phibar
        total = total + (phi / rho) * search
        image = image + (phi / rho) * search_image
        turn = theta / rho
        search = point - turn * search
        alpha = alpha_next
    solution = lax.dynamic_slice_in_dim(total, c * col_count, col_count, 1)
    return (solution, right_sides - image)


def solution(mesh):
    in_specs = (P("rows", "cols"), P("rows"), P("rows", None), P(None, "rows"))
    out_specs = (P(None, "cols"), P(None, "rows"))
    return jax.shard_map(local, mesh=mesh, in_specs=in_specs, out_specs=out_specs, check_vma=False)
```
